32 devices in a mesh: section: 4 (over y, x), dev: 8 (over z, core).
Axes of the slice: x: 2, y: 2, z: 4, core: 2. Of those that a mesh axis runs over, the one named last changes fastest.
Arguments:
- late_sent: bfloat16 [4, 784, 1024], P('section', 'dev'), may hold values from -5 to 5
- entry_rows: bfloat16 [784, 1024], P('dev'), may hold values from -5 to 5
- gain_first: float32 [4, 1024], P('section'), may hold values from 0.1 to 1.9
- shift_first: float32 [4, 1024], P('section'), may hold values from -3 to 3
- expand_late: bfloat16 [4, 1024, 4096], P('section', None, 'dev'), may hold values from -0.1875 to 0.1875
- gain_inner: float32 [4, 4096], P('section', 'dev'), may hold values from 0.1 to 1.9
- shift_inner: float32 [4, 4096], P('section', 'dev'), may hold values from -3 to 3
- reduce_late: bfloat16 [4, 4096, 1024], P('section', 'dev'), may hold values from -0.09375 to 0.09375
- early_saved: bfloat16 [4, 12544, 256], P('section', 'dev'), may hold values from -6 to 6
- upstream_grad: bfloat16 [4, 12544, 256], P('section', 'dev'), may hold values from -6 to 6
- exit_grad: bfloat16 [12544, 256], P('dev'), may hold values from -6 to 6
- expand_early: bfloat16 [4, 256, 1024], P('section'), may hold values from -0.375 to 0.375
- reduce_early: bfloat16 [4, 1024, 256], P('section'), may hold values from -0.1875 to 0.1875
Outputs:
- late_out: bfloat16 [4, 784, 1024], P('section', 'dev')
- input_grad: bfloat16 [4, 12544, 256], P('section', 'dev')
- grad_expand: float32 [4, 256, 1024], P('section')
- grad_reduce: float32 [4, 1024, 256], P('section')
The draws below stay inside these ranges and needn't reach their ends.
All inputs are finite; a program needn't handle non-finite values.
Results may differ from the reference program's by a relative error of at most 0.02.
Values may be sent and summed in bfloat16 or wider, within the bound.
A program may use at most 128 MiB of HBM per device.

```python
import math
import jax
import jax.numpy as jnp
from jax import lax

CE = 256
FE = 1024
CL = 1024
FL = 4096
SECTIONS = 4
HID_DEV = 512
E_ROWS = 12544
L_ROWS = 784
N_DEV = 8


def scaled_rows(key, leading):
    keys = jax.random.split(key, 4)
    shape = (leading, L_ROWS, CL)
    base = jnp.clip(jax.random.normal(keys[0], shape, jnp.float32), -4.0, 4.0)
    weight = 0.5
    rise = 6.0
    trend = jnp.exp(math.log(rise) * jnp.arange(L_ROWS, dtype=jnp.float32) / L_ROWS).reshape(1, L_ROWS, 1)
    row_factor = jnp.exp(jax.random.uniform(keys[1], (leading, L_ROWS, 1), jnp.float32, 0.0, math.log(2.0)))
    column_factor = jnp.exp(jax.random.uniform(keys[2], (leading, 1, CL), jnp.float32, 0.0, math.log(10.0)))
    offset = jnp.clip(jax.random.normal(keys[3], (leading, 1, CL), jnp.float32), -2.0, 2.0) * weight
    return 0.005 * (base * row_factor + offset) * trend * column_factor


def draw_late_sent(key, part):
    return scaled_rows(jax.random.fold_in(key, 101), SECTIONS).astype(jnp.bfloat16)


def draw_entry_rows(key, part):
    return scaled_rows(jax.random.fold_in(key, 202), 1)[0].astype(jnp.bfloat16)


def block_scale(own_key, shape, shards, smallest, top_value):
    loudness = 1.0
    for position, parts in shards:
        steps = jax.random.uniform(jax.random.fold_in(jax.random.fold_in(own_key, 6), position), (parts,), jnp.float32, smallest / len(shards), top_value / len(shards))
        loudness = loudness * jnp.repeat(jnp.exp(steps), shape[position] // parts).reshape((-1,) + (1,) * (len(shape) - 1 - position))
    return loudness


def scatter_about(own_key, extent, deviation, reach, cuts=(), held_as=jnp.bfloat16):
    values = jax.random.normal(own_key, extent, jnp.float32) * deviation
    if len(cuts) > 0:
        values = block_scale(own_key, extent, cuts, -0.22, 0.18) * values
    return jnp.clip(values, min=-reach, max=reach).astype(held_as)


def setup_inputs(seed: int = 0) -> dict:
    key_of = jax.random.split(jax.random.key(seed), 14)
    return {
        "late_sent": draw_late_sent(jax.random.fold_in(key_of[13], 71), 0),
        "entry_rows": draw_entry_rows(jax.random.fold_in(key_of[13], 71), 0),
        "gain_first": jnp.clip(1.0 + 0.18 * jax.random.normal(key_of[2], (SECTIONS, CL), jnp.float32), 0.1, 1.9),
        "shift_first": scatter_about(key_of[3], (SECTIONS, CL), 0.5, 3.0, ((0, 4),), jnp.float32),
        "expand_late": scatter_about(key_of[4], (SECTIONS, CL, FL), CL ** -0.5, 0.1875, ((0, 4), (2, 8))),
        "gain_inner": jnp.clip(1.0 + 0.18 * jax.random.normal(key_of[5], (SECTIONS, FL), jnp.float32), 0.1, 1.9),
        "shift_inner": scatter_about(key_of[6], (SECTIONS, FL), 0.5, 3.0, ((0, 4), (1, 8)), jnp.float32),
        "reduce_late": scatter_about(key_of[7], (SECTIONS, FL, CL), FL ** -0.5, 0.09375, ((0, 4), (1, 8))),
        "early_saved": scatter_about(key_of[8], (SECTIONS, E_ROWS, CE), 1.0, 6.0, ((0, 4), (1, 8))),
        "upstream_grad": scatter_about(key_of[9], (SECTIONS, E_ROWS, CE), 1.0, 6.0, ((0, 4), (1, 8))),
        "exit_grad": scatter_about(key_of[10], (E_ROWS, CE), 1.0, 6.0, ((0, 8),)),
        "expand_early": scatter_about(key_of[11], (SECTIONS, CE, FE), CE ** -0.5, 0.375, ((0, 4),)),
        "reduce_early": scatter_about(key_of[12], (SECTIONS, FE, CE), FE ** -0.5, 0.1875, ((0, 4),)),
    }


epsilon = 1e-05

def affine(sums, squares, count, gain, shift):
    average = sums / count
    second = squares / count
    spread = gain * lax.rsqrt(second - average * average + epsilon)
    return (spread, shift - average * spread)

def silu_slope(values):
    sigma = jax.nn.sigmoid(values)
    return sigma * (1.0 + values * (1.0 - sigma))

def late_block(inputs, gain_first, shift_first, expand, gain_inner, shift_inner, reduce_weight):
    count = inputs.shape[0]
    values = inputs.astype(jnp.float32)
    spread, offset = affine(lax.optimization_barrier(jnp.sum(values, axis=0)), lax.optimization_barrier(jnp.sum(values * values, axis=0)), count, gain_first, shift_first)
    first = jax.nn.silu(values * spread + offset).astype(jnp.bfloat16)
    inner = jnp.dot(first, expand, preferred_element_type=jnp.float32)
    spread_two, offset_two = affine(lax.optimization_barrier(jnp.sum(inner, axis=0)), lax.optimization_barrier(jnp.sum(inner * inner, axis=0)), count, gain_inner, shift_inner)
    hidden = jax.nn.silu(inner * spread_two + offset_two).astype(jnp.bfloat16)

    def add_group(total, group):
        start = (group * HID_DEV).astype(jnp.int32)
        term = jnp.dot(lax.dynamic_slice_in_dim(hidden, start, HID_DEV, 1), lax.dynamic_slice_in_dim(reduce_weight, start, HID_DEV, 0), preferred_element_type=jnp.float32)
        rounded = lax.optimization_barrier(term.astype(jnp.bfloat16))
        return (total + rounded.astype(jnp.float32), None)
    total, unused = lax.scan(add_group, jnp.zeros((count, CL), jnp.float32), jnp.arange(N_DEV, dtype=jnp.int32))
    return (values + total).astype(jnp.bfloat16)

def early_block(saved, grad, expand, reduce_weight):
    pre = jnp.dot(saved, expand, preferred_element_type=jnp.float32)
    hidden = jax.nn.silu(pre).astype(jnp.bfloat16)
    back = lax.dot_general(grad, reduce_weight, (((1,), (1,)), ((), ())), preferred_element_type=jnp.float32)
    slope = (back * silu_slope(pre)).astype(jnp.bfloat16)
    result = grad.astype(jnp.float32) + lax.dot_general(slope, expand, (((1,), (1,)), ((), ())), preferred_element_type=jnp.float32)
    grad_expand = lax.dot_general(saved, slope, (((0,), (0,)), ((), ())), preferred_element_type=jnp.float32)
    grad_reduce = lax.dot_general(hidden, grad, (((0,), (0,)), ((), ())), preferred_element_type=jnp.float32)
    return (result.astype(jnp.bfloat16), grad_expand, grad_reduce)

def reference(late_sent, entry_rows, gain_first, shift_first, expand_late, gain_inner, shift_inner, reduce_late, early_saved, upstream_grad, exit_grad, expand_early, reduce_early):
    late_in = jnp.concatenate([entry_rows[None], late_sent[:-1]], axis=0)
    grad_in = jnp.concatenate([upstream_grad[1:], exit_grad[None]], axis=0)
    late_out = lax.map(lambda items: late_block(*items), (late_in, gain_first, shift_first, expand_late, gain_inner, shift_inner, reduce_late))
    input_grad, grad_expand, grad_reduce = lax.map(lambda items: early_block(*items), (early_saved, grad_in, expand_early, reduce_early))
    factor = 1.0 / math.sqrt(E_ROWS)
    return (late_out, input_grad, grad_expand * factor, grad_reduce * factor)
```

```python
import functools
import math

import jax
import jax.numpy as jnp
from jax import lax
from jax.experimental import pallas as pl
from jax.experimental.pallas import tpu as pltpu
from jax.sharding import PartitionSpec as P

MESH = pl.DeviceIdType.MESH
epsilon = 1e-05
F32 = jnp.float32
BF16 = jnp.bfloat16


def sigmoid(x):
    return 0.5 * jnp.tanh(0.5 * x) + 0.5


def affine(sums, squares, count, gain, shift):
    average = sums / count
    second = squares / count
    spread = gain * lax.rsqrt(second - average * average + epsilon)
    return spread, shift - average * spread


def dot(a, b, ca=1, cb=0):
    return lax.dot_general(a, b, (((ca,), (cb,)), ((), ())), preferred_element_type=F32)


def kernel(
    sections, n_dev, chunk,
    late_hbm, entry_hbm, gain1, shift1, wexp_hbm, gain2, shift2, wred_hbm,
    saved_hbm, up_hbm, exit_hbm, eexp_hbm, ered_hbm,
    late_out, input_grad, wout,
    lbuf, first, hidden, part, prx, ltx, lrx,
    wexp, wred, saved, grad, eexp, ered, act, dsl, slope,
    gsum, gtx, gprx, wtx, wrx, abuf,
    loc_sem, perm_send, perm_recv, gp_send, gp_recv,
    ag_s, ag_r, agp_s, agp_r, px_s, px_r, rs_s, rs_r,
    gx_s, gx_r, wrs_s, wrs_r, wag_s, wag_r, wagp_s, wagp_r,
):
    Q = n_dev // 2
    s = lax.axis_index("section")
    d = lax.axis_index("dev")
    q = d // 2
    c = lax.rem(d, 2)
    other = 1 - c
    partner = q * 2 + other
    rows = late_hbm.shape[0]
    half = late_hbm.shape[1] // 2
    padded = first.shape[0] // n_dev
    e_rows = saved_hbm.shape[0]
    steps = e_rows // chunk
    total_rows = rows * n_dev
    hid = wexp.shape[1]

    def at_chip(offset):
        return lax.rem(q + offset + 2 * Q, Q)

    sgn = (1, -1)
    nxt = tuple(at_chip(g) * 2 + c for g in sgn)

    barrier = pltpu.get_barrier_semaphore()
    for dev in (nxt[0], nxt[1], partner):
        pl.semaphore_signal(barrier, inc=1, device_id=(s, dev), device_id_type=MESH)

    @pl.when(s > 0)
    def _():
        pl.semaphore_signal(barrier, inc=1, device_id=(s - 1, d), device_id_type=MESH)

    @pl.when(s < sections - 1)
    def _():
        pl.semaphore_signal(barrier, inc=1, device_id=(s + 1, d), device_id_type=MESH)

    local = [
        pltpu.make_async_copy(src, dst, loc_sem.at[i])
        for i, (src, dst) in enumerate(
            ((saved_hbm, saved), (eexp_hbm, eexp), (ered_hbm, ered), (wexp_hbm, wexp), (wred_hbm, wred))
        )
    ]
    for copy in local:
        copy.start()

    pl.semaphore_wait(barrier, 3 + jnp.minimum(s, 1) + jnp.minimum(sections - 1 - s, 1))

    def remote(src, dst, send, recv, section, dev):
        return pltpu.make_async_remote_copy(
            src_ref=src, dst_ref=dst, send_sem=send, recv_sem=recv,
            device_id=(section, dev), device_id_type=MESH,
        )

    def cols(h):
        return pl.ds(h * half, half)

    def late_copy(h):
        return remote(
            late_hbm.at[:, cols(h)], lbuf.at[h, d], perm_send.at[h], perm_recv.at[h],
            jnp.minimum(s + 1, sections - 1), d,
        )

    def entry_copy(h):
        return pltpu.make_async_copy(entry_hbm.at[:, cols(h)], lbuf.at[h, d], perm_recv.at[h])

    def chunk_rows(j):
        return pl.ds(j * chunk, chunk)

    def grad_copy(j):
        return remote(
            up_hbm.at[chunk_rows(j)], grad.at[chunk_rows(j)], gp_send.at[j], gp_recv.at[j],
            jnp.maximum(s - 1, 0), d,
        )

    def exit_copy(j):
        return pltpu.make_async_copy(exit_hbm.at[chunk_rows(j)], grad.at[chunk_rows(j)], gp_recv.at[j])

    @pl.when(s < sections - 1)
    def _():
        for h in range(2):
            late_copy(h).start()

    @pl.when(s == 0)
    def _():
        for h in range(2):
            entry_copy(h).start()

    @pl.when(s > 0)
    def _():
        for j in range(steps):
            grad_copy(j).start()

    @pl.when(s == sections - 1)
    def _():
        for j in range(steps):
            exit_copy(j).start()

    def ring_gather(buf, ss, rr, ps, pr):
        def owner(h, t, lane):
            return at_chip(-sgn[h] * t) * 2 + lane

        def hop(h, t):
            piece = buf.at[h, owner(h, t, c)]
            return remote(piece, piece, ss.at[h, t], rr.at[h, t], s, nxt[h])

        def arrival(h, t):
            piece = buf.at[h, owner(h, t + 1, c)]
            return remote(piece, piece, ss.at[h, t], rr.at[h, t], s, nxt[h])

        def share(h, t, lane):
            piece = buf.at[h, owner(h, t, lane)]
            return remote(piece, piece, ps.at[h, t], pr.at[h, t], s, partner)

        def start(h):
            hop(h, 0).start()
            share(h, 0, c).start()

        def advance(h, t):
            arrival(h, t).wait_recv()
            if t + 1 < Q - 1:
                hop(h, t + 1).start()
            share(h, t + 1, c).start()

        def finish():
            for h in range(2):
                for t in range(Q):
                    share(h, t, other).wait_recv()

        def drain():
            for h in range(2):
                for t in range(Q - 1):
                    hop(h, t).wait_send()
                for t in range(Q):
                    share(h, t, c).wait_send()

        return start, advance, finish, drain

    def ring_scatter(mine, tx, rx, ss, rr):
        def hop(h, t):
            return remote(tx.at[h, t], rx.at[h, t], ss.at[h, t], rr.at[h, t], s, nxt[h])

        def start(h):
            tx[h, 0] = mine(h, at_chip(-sgn[h])).astype(BF16)
            hop(h, 0).start()

        def advance(h, t):
            hop(h, t).wait_recv()
            value = mine(h, at_chip(-sgn[h] * (t + 2))) + rx[h, t].astype(F32)
            if t == Q - 2:
                return value
            tx[h, t + 1] = value.astype(BF16)
            hop(h, t + 1).start()

        def drain():
            for h in range(2):
                for t in range(Q - 1):
                    hop(h, t).wait_send()

        return start, advance, drain

    def forward(j):
        at = chunk_rows(j)
        pre = dot(saved[at], eexp[...])
        sigma = sigmoid(pre)
        value = pre * sigma
        act[at] = value.astype(BF16)
        dsl[at] = sigma * (1.0 + pre - value)

    def backward(j):
        at = chunk_rows(j)

        @pl.when(s < sections - 1)
        def _():
            grad_copy(j).wait_recv()

        @pl.when(s == sections - 1)
        def _():
            exit_copy(j).wait()

        g = grad[at]
        back = dot(g, ered[...], 1, 1)
        sl = (back * dsl[at]).astype(BF16)
        slope[at] = sl
        input_grad[at] = (g.astype(F32) + dot(sl, eexp[...], 1, 1)).astype(BF16)

    local[0].wait()
    local[1].wait()
    fwd = 0
    first_part = max(steps // 2, 1)
    for j in range(first_part):
        forward(j)
    fwd = first_part

    @pl.when(s == 0)
    def _():
        for h in range(2):
            entry_copy(h).wait()

    @pl.when(s > 0)
    def _():
        for h in range(2):
            late_copy(h).wait_recv()

    ag_start, ag_advance, ag_finish, ag_drain = ring_gather(lbuf, ag_s, ag_r, agp_s, agp_r)
    for h in range(2):
        ag_start(h)
    for dev in range(n_dev):
        first[pl.ds((dev + 1) * padded - 16, 16), :] = jnp.zeros((16, first.shape[1]), BF16)
    for t in range(Q - 1):
        if fwd < steps:
            forward(fwd)
            fwd += 1
        for h in range(2):
            ag_advance(h, t)
    for j in range(fwd, steps):
        forward(j)
    ag_finish()

    for h in range(2):
        total = jnp.zeros((1, half), F32)
        squares = jnp.zeros((1, half), F32)
        for dev in range(n_dev):
            v = lbuf[h, dev].astype(F32)
            total += jnp.sum(v, axis=0, keepdims=True)
            squares += jnp.sum(v * v, axis=0, keepdims=True)
        spread, offset = affine(total, squares, total_rows, gain1[:, cols(h)], shift1[:, cols(h)])
        for dev in range(n_dev):
            v = lbuf[h, dev].astype(F32) * spread + offset
            first[pl.ds(dev * padded, rows), cols(h)] = (v * sigmoid(v)).astype(BF16)

    local[3].wait()
    local[4].wait()
    width = min(256, hid)
    for n in range(hid // width):
        at = pl.ds(n * width, width)
        inner = dot(first[...], wexp[:, at])
        spread, offset = affine(
            jnp.sum(inner, axis=0, keepdims=True),
            jnp.sum(inner * inner, axis=0, keepdims=True),
            total_rows, gain2[:, at], shift2[:, at],
        )
        v = inner * spread + offset
        hidden[:, at] = (v * sigmoid(v)).astype(BF16)

    def pair_copy(h):
        return remote(part.at[other, h], prx.at[h], px_s.at[h], px_r.at[h], s, partner)

    tile = min(256, half)
    for h in range(2):
        for n in range(half // tile):
            value = dot(hidden[...], wred[:, pl.ds(h * half + n * tile, tile)]).astype(BF16)
            for dev in range(n_dev):
                part[dev % 2, h, dev // 2, :, pl.ds(n * tile, tile)] = value[dev * padded:dev * padded + rows]
        pair_copy(h).start()

    def late_term(h, k):
        return part[c, h, k].astype(F32) + prx[h, k].astype(F32)

    rs_start, rs_advance, rs_drain = ring_scatter(late_term, ltx, lrx, rs_s, rs_r)
    for h in range(2):
        pair_copy(h).wait_recv()
        rs_start(h)

    local[2].wait()
    bwd = 0
    per = -(-steps // (Q - 1))
    for t in range(Q - 1):
        for j in range(bwd, min(bwd + per, steps)):
            backward(j)
        bwd = min(bwd + per, steps)
        for h in range(2):
            value = rs_advance(h, t)
            if t == Q - 2:
                late_out[:, cols(h)] = (lbuf[h, d].astype(F32) + value).astype(BF16)

    depth = gsum.shape[2]
    wide = eexp.shape[1]
    for n in range(wide // 256):
        at = pl.ds(n * 256, 256)
        gsum[0, :, :, at] = dot(saved[...], slope[:, at], 0, 0).reshape(Q, depth, 256)
        gsum[1, :, :, at] = dot(grad[...], act[:, at], 0, 0).reshape(Q, depth, 256)
    gtx[...] = gsum[other].astype(BF16)
    gx = remote(gtx, gprx, gx_s, gx_r, s, partner)
    gx.start()
    gx.wait_recv()
    whalf = wide // 2

    def wcols(h):
        return pl.ds(h * whalf, whalf)

    def weight_term(h, k):
        return gsum[c, k, :, wcols(h)] + gprx[k, :, wcols(h)].astype(F32)

    ws_start, ws_advance, ws_drain = ring_scatter(weight_term, wtx, wrx, wrs_s, wrs_r)
    wg_start, wg_advance, wg_finish, wg_drain = ring_gather(abuf, wag_s, wag_r, wagp_s, wagp_r)
    factor = 1.0 / math.sqrt(e_rows * n_dev)
    for h in range(2):
        ws_start(h)
    for t in range(Q - 1):
        for h in range(2):
            value = ws_advance(h, t)
            if t == Q - 2:
                abuf[h, d] = (value * factor).astype(BF16)
                wg_start(h)
    for t in range(Q - 1):
        for h in range(2):
            wg_advance(h, t)
    wg_finish()
    for h in range(2):
        for k in range(Q):
            for lane in range(2):
                wout[lane, k, :, wcols(h)] = abuf[h, 2 * k + lane].astype(F32)

    @pl.when(s < sections - 1)
    def _():
        for h in range(2):
            late_copy(h).wait_send()

    @pl.when(s > 0)
    def _():
        for j in range(steps):
            grad_copy(j).wait_send()

    ag_drain()
    for h in range(2):
        pair_copy(h).wait_send()
    rs_drain()
    gx.wait_send()
    ws_drain()
    wg_drain()


def shards(
    sections, n_dev,
    late_sent, entry_rows, gain_first, shift_first, expand_late, gain_inner, shift_inner,
    reduce_late, early_saved, upstream_grad, exit_grad, expand_early, reduce_early,
):
    rows, cl = entry_rows.shape
    e_rows, ce = exit_grad.shape
    fe = expand_early.shape[2]
    hid = expand_late.shape[2]
    Q = n_dev // 2
    half = cl // 2
    padded = -(-rows // 16) * 16
    chunk = max(k for k in range(16, 257, 16) if e_rows % k == 0)
    steps = e_rows // chunk
    depth = ce // Q
    any_spec = pl.BlockSpec(memory_space=pl.ANY)
    vm = pl.BlockSpec(memory_space=pltpu.VMEM)
    V = pltpu.VMEM
    dma = pltpu.SemaphoreType.DMA
    ring = [dma((2, Q - 1)), dma((2, Q - 1))]
    late_out, input_grad, wout = pl.pallas_call(
        functools.partial(kernel, sections, n_dev, chunk),
        out_shape=(
            jax.ShapeDtypeStruct((rows, cl), BF16),
            jax.ShapeDtypeStruct((e_rows, ce), BF16),
            jax.ShapeDtypeStruct((2, Q, depth, fe), F32),
        ),
        in_specs=[any_spec, any_spec, vm, vm, any_spec, vm, vm] + [any_spec] * 6,
        out_specs=(vm, vm, vm),
        scratch_shapes=[
            V((2, n_dev, rows, half), BF16),
            V((n_dev * padded, cl), BF16),
            V((n_dev * padded, hid), BF16),
            V((2, 2, Q, rows, half), BF16),
            V((2, Q, rows, half), BF16),
            V((2, Q - 1, rows, half), BF16),
            V((2, Q - 1, rows, half), BF16),
            V((cl, hid), BF16),
            V((hid, cl), BF16),
            V((e_rows, ce), BF16),
            V((e_rows, ce), BF16),
            V((ce, fe), BF16),
            V((fe, ce), BF16),
            V((e_rows, fe), BF16),
            V((e_rows, fe), F32),
            V((e_rows, fe), BF16),
            V((2, Q, depth, fe), F32),
            V((Q, depth, fe), BF16),
            V((Q, depth, fe), BF16),
            V((2, Q - 1, depth, fe // 2), BF16),
            V((2, Q - 1, depth, fe // 2), BF16),
            V((2, n_dev, depth, fe // 2), BF16),
            dma((5,)), dma((2,)), dma((2,)), dma((steps,)), dma((steps,)),
            *ring, dma((2, Q)), dma((2, Q)), dma((2,)), dma((2,)), *ring,
            dma, dma, *ring, *ring, dma((2, Q)), dma((2, Q)),
        ],
        compiler_params=pltpu.CompilerParams(
            collective_id=0, has_side_effects=True, vmem_limit_bytes=60 * 1024 * 1024
        ),
        name="relay",
    )(
        late_sent[0], entry_rows, gain_first, shift_first, expand_late[0], gain_inner, shift_inner,
        reduce_late[0], early_saved[0], upstream_grad[0], exit_grad, expand_early[0], reduce_early[0],
    )
    wout = wout.reshape(2, ce, fe)
    return late_out[None], input_grad[None], wout[0][None], wout[1].T[None]


def solution(mesh):
    sections, n_dev = mesh.shape["section"], mesh.shape["dev"]
    sd, dd = P("section", "dev", None), P("dev", None)
    rep, one = P("section", None, None), P("section", None)
    in_specs = (
        sd, dd, one, one, P("section", None, "dev"), P("section", "dev"), P("section", "dev"),
        sd, sd, sd, dd, rep, rep,
    )
    return jax.shard_map(
        functools.partial(shards, sections, n_dev), mesh=mesh, in_specs=in_specs,
        out_specs=(sd, sd, rep, rep), check_vma=False,
    )
```

```python
import functools
import math

import jax
import jax.numpy as jnp
from jax import lax
from jax.experimental import pallas as pl
from jax.experimental.pallas import tpu as pltpu
from jax.sharding import PartitionSpec as P

MESH = pl.DeviceIdType.MESH
epsilon = 1e-05
F32 = jnp.float32
BF16 = jnp.bfloat16


def sigmoid(x):
    return 0.5 * jnp.tanh(0.5 * x) + 0.5


def affine(sums, squares, count, gain, shift):
    average = sums / count
    second = squares / count
    spread = gain * lax.rsqrt(second - average * average + epsilon)
    return spread, shift - average * spread


def dot(a, b, ca=1, cb=0):
    return lax.dot_general(a, b, (((ca,), (cb,)), ((), ())), preferred_element_type=F32)


def kernel(
    sections, n_dev, chunk,
    late_hbm, entry_hbm, gain1, shift1, wexp_hbm, gain2, shift2, wred_hbm,
    saved_hbm, up_hbm, exit_hbm, eexp_hbm, ered_hbm,
    late_out, input_grad, gexp_out, gred_out,
    lbuf, first, hidden, part, prx, ltx, lrx,
    wexp, wred, saved, grad, eexp, ered, act, dsl, slope,
    gsum, gtx, gprx, wtx, wrx, abuf, turn,
    loc_sem, perm_send, perm_recv, gp_send, gp_recv,
    ag_s, ag_r, agp_s, agp_r, px_s, px_r, rs_s, rs_r,
    gx_s, gx_r, wrs_s, wrs_r, wag_s, wag_r, wagp_s, wagp_r,
):
    Q = n_dev // 2
    s = lax.axis_index("section")
    d = lax.axis_index("dev")
    q = d // 2
    c = lax.rem(d, 2)
    other = 1 - c
    partner = q * 2 + other
    rows = late_hbm.shape[0]
    half = late_hbm.shape[1] // 2
    padded = first.shape[0] // n_dev
    e_rows = saved_hbm.shape[0]
    steps = e_rows // chunk
    total_rows = rows * n_dev
    hid = wexp.shape[1]

    def at_chip(offset):
        return lax.rem(q + offset + 2 * Q, Q)

    sgn = (1, -1)
    nxt = tuple(at_chip(g) * 2 + c for g in sgn)

    barrier = pltpu.get_barrier_semaphore()
    for dev in (nxt[0], nxt[1], partner):
        pl.semaphore_signal(barrier, inc=1, device_id=(s, dev), device_id_type=MESH)

    @pl.when(s > 0)
    def _():
        pl.semaphore_signal(barrier, inc=1, device_id=(s - 1, d), device_id_type=MESH)

    @pl.when(s < sections - 1)
    def _():
        pl.semaphore_signal(barrier, inc=1, device_id=(s + 1, d), device_id_type=MESH)

    local = [
        pltpu.make_async_copy(src, dst, loc_sem.at[i])
        for i, (src, dst) in enumerate(
            ((saved_hbm, saved), (eexp_hbm, eexp), (ered_hbm, ered), (wexp_hbm, wexp), (wred_hbm, wred))
        )
    ]
    for copy in local:
        copy.start()

    pl.semaphore_wait(barrier, 3 + jnp.minimum(s, 1) + jnp.minimum(sections - 1 - s, 1))

    def remote(src, dst, send, recv, section, dev):
        return pltpu.make_async_remote_copy(
            src_ref=src, dst_ref=dst, send_sem=send, recv_sem=recv,
            device_id=(section, dev), device_id_type=MESH,
        )

    def cols(h):
        return pl.ds(h * half, half)

    def late_copy(h):
        return remote(
            late_hbm.at[:, cols(h)], lbuf.at[h, d], perm_send.at[h], perm_recv.at[h],
            jnp.minimum(s + 1, sections - 1), d,
        )

    def entry_copy(h):
        return pltpu.make_async_copy(entry_hbm.at[:, cols(h)], lbuf.at[h, d], perm_recv.at[h])

    def chunk_rows(j):
        return pl.ds(j * chunk, chunk)

    def grad_copy(j):
        return remote(
            up_hbm.at[chunk_rows(j)], grad.at[chunk_rows(j)], gp_send.at[j], gp_recv.at[j],
            jnp.maximum(s - 1, 0), d,
        )

    def exit_copy(j):
        return pltpu.make_async_copy(exit_hbm.at[chunk_rows(j)], grad.at[chunk_rows(j)], gp_recv.at[j])

    @pl.when(s < sections - 1)
    def _():
        for h in range(2):
            late_copy(h).start()

    @pl.when(s == 0)
    def _():
        for h in range(2):
            entry_copy(h).start()

    @pl.when(s > 0)
    def _():
        for j in range(steps):
            grad_copy(j).start()

    @pl.when(s == sections - 1)
    def _():
        for j in range(steps):
            exit_copy(j).start()

    def ring_gather(buf, ss, rr, ps, pr):
        def owner(h, t, lane):
            return at_chip(-sgn[h] * t) * 2 + lane

        def hop(h, t):
            piece = buf.at[h, owner(h, t, c)]
            return remote(piece, piece, ss.at[h, t], rr.at[h, t], s, nxt[h])

        def arrival(h, t):
            piece = buf.at[h, owner(h, t + 1, c)]
            return remote(piece, piece, ss.at[h, t], rr.at[h, t], s, nxt[h])

        def share(h, t, lane):
            piece = buf.at[h, owner(h, t, lane)]
            return remote(piece, piece, ps.at[h, t], pr.at[h, t], s, partner)

        def start(h):
            hop(h, 0).start()
            share(h, 0, c).start()

        def advance(h, t):
            arrival(h, t).wait_recv()
            if t + 1 < Q - 1:
                hop(h, t + 1).start()
            share(h, t + 1, c).start()

        def finish():
            for h in range(2):
                for t in range(Q):
                    share(h, t, other).wait_recv()

        def drain():
            for h in range(2):
                for t in range(Q - 1):
                    hop(h, t).wait_send()
                for t in range(Q):
                    share(h, t, c).wait_send()

        return start, advance, finish, drain

    def ring_scatter(mine, tx, rx, ss, rr):
        def hop(h, t):
            return remote(tx.at[h, t], rx.at[h, t], ss.at[h, t], rr.at[h, t], s, nxt[h])

        def start(h):
            tx[h, 0] = mine(h, at_chip(-sgn[h])).astype(BF16)
            hop(h, 0).start()

        def advance(h, t):
            hop(h, t).wait_recv()
            value = mine(h, at_chip(-sgn[h] * (t + 2))) + rx[h, t].astype(F32)
            if t == Q - 2:
                return value
            tx[h, t + 1] = value.astype(BF16)
            hop(h, t + 1).start()

        def drain():
            for h in range(2):
                for t in range(Q - 1):
                    hop(h, t).wait_send()

        return start, advance, drain

    def forward(j):
        at = chunk_rows(j)
        pre = dot(saved[at], eexp[...])
        sigma = sigmoid(pre)
        value = pre * sigma
        act[at] = value.astype(BF16)
        dsl[at] = sigma * (1.0 + pre - value)

    def backward(j):
        at = chunk_rows(j)

        @pl.when(s < sections - 1)
        def _():
            grad_copy(j).wait_recv()

        @pl.when(s == sections - 1)
        def _():
            exit_copy(j).wait()

        g = grad[at]
        back = dot(g, ered[...], 1, 1)
        sl = (back * dsl[at]).astype(BF16)
        slope[at] = sl
        input_grad[at] = (g.astype(F32) + dot(sl, eexp[...], 1, 1)).astype(BF16)

    local[0].wait()
    local[1].wait()
    fwd = 0
    first_part = max(steps // 2, 1)
    for j in range(first_part):
        forward(j)
    fwd = first_part

    @pl.when(s == 0)
    def _():
        for h in range(2):
            entry_copy(h).wait()

    @pl.when(s > 0)
    def _():
        for h in range(2):
            late_copy(h).wait_recv()

    ag_start, ag_advance, ag_finish, ag_drain = ring_gather(lbuf, ag_s, ag_r, agp_s, agp_r)
    for h in range(2):
        ag_start(h)
    for dev in range(n_dev):
        first[pl.ds((dev + 1) * padded - 16, 16), :] = jnp.zeros((16, first.shape[1]), BF16)
    for t in range(Q - 1):
        if fwd < steps:
            forward(fwd)
            fwd += 1
        if t == Q - 2:
            for j in range(fwd, steps):
                forward(j)
            fwd = steps
        for h in range(2):
            ag_advance(h, t)

    local[2].wait()
    for j in range(steps):
        backward(j)
    depth = gsum.shape[2]
    wide = eexp.shape[1]
    for n in range(wide // 256):
        at = pl.ds(n * 256, 256)
        gsum[0, :, :, at] = dot(saved[...], slope[:, at], 0, 0).reshape(Q, depth, 256)
        gsum[1, :, :, at] = dot(grad[...], act[:, at], 0, 0).reshape(Q, depth, 256)
    gtx[...] = gsum[other].astype(BF16)
    gx = remote(gtx, gprx, gx_s, gx_r, s, partner)
    gx.start()
    ag_finish()

    for h in range(2):
        total = jnp.zeros((1, half), F32)
        squares = jnp.zeros((1, half), F32)
        for dev in range(n_dev):
            v = lbuf[h, dev].astype(F32)
            total += jnp.sum(v, axis=0, keepdims=True)
            squares += jnp.sum(v * v, axis=0, keepdims=True)
        spread, offset = affine(total, squares, total_rows, gain1[:, cols(h)], shift1[:, cols(h)])
        for dev in range(n_dev):
            v = lbuf[h, dev].astype(F32) * spread + offset
            first[pl.ds(dev * padded, rows), cols(h)] = (v * sigmoid(v)).astype(BF16)

    gx.wait_recv()
    whalf = wide // 2

    def wcols(h):
        return pl.ds(h * whalf, whalf)

    def weight_term(h, k):
        return gsum[c, k, :, wcols(h)] + gprx[k, :, wcols(h)].astype(F32)

    ws_start, ws_advance, ws_drain = ring_scatter(weight_term, wtx, wrx, wrs_s, wrs_r)
    wg_start, wg_advance, wg_finish, wg_drain = ring_gather(abuf, wag_s, wag_r, wagp_s, wagp_r)
    factor = 1.0 / math.sqrt(e_rows * n_dev)

    def weight_step(t):
        for h in range(2):
            value = ws_advance(h, t)
            if t == Q - 2:
                abuf[h, d] = (value * factor).astype(BF16)
                wg_start(h)

    for h in range(2):
        ws_start(h)

    local[3].wait()
    local[4].wait()
    width = min(256, hid)
    for n in range(hid // width):
        at = pl.ds(n * width, width)
        inner = dot(first[...], wexp[:, at])
        spread, offset = affine(
            jnp.sum(inner, axis=0, keepdims=True),
            jnp.sum(inner * inner, axis=0, keepdims=True),
            total_rows, gain2[:, at], shift2[:, at],
        )
        v = inner * spread + offset
        hidden[:, at] = (v * sigmoid(v)).astype(BF16)

    def pair_copy(h):
        return remote(part.at[other, h], prx.at[h], px_s.at[h], px_r.at[h], s, partner)

    tile = min(256, half)
    for h in range(2):
        for n in range(half // tile):
            value = dot(hidden[...], wred[:, pl.ds(h * half + n * tile, tile)]).astype(BF16)
            for dev in range(n_dev):
                part[dev % 2, h, dev // 2, :, pl.ds(n * tile, tile)] = value[dev * padded:dev * padded + rows]
        pair_copy(h).start()

    weight_step(0)

    def late_term(h, k):
        return part[c, h, k].astype(F32) + prx[h, k].astype(F32)

    rs_start, rs_advance, rs_drain = ring_scatter(late_term, ltx, lrx, rs_s, rs_r)
    for h in range(2):
        pair_copy(h).wait_recv()
        rs_start(h)

    for t in range(1, Q - 1):
        weight_step(t)
    for t in range(Q - 1):
        for h in range(2):
            value = rs_advance(h, t)
            if t == Q - 2:
                late_out[:, cols(h)] = (lbuf[h, d].astype(F32) + value).astype(BF16)
        for h in range(2):
            wg_advance(h, t)
    wg_finish()
    for h in range(2):
        for k in range(Q):
            at = pl.ds(k * depth, depth)
            gexp_out[at, wcols(h)] = abuf[h, 2 * k]
            turn[at, wcols(h)] = abuf[h, 2 * k + 1].astype(F32)
    for n in range(wide // 256):
        at = pl.ds(n * 256, 256)
        gred_out[at, :] = turn[:, at].T.astype(BF16)

    @pl.when(s < sections - 1)
    def _():
        for h in range(2):
            late_copy(h).wait_send()

    @pl.when(s > 0)
    def _():
        for j in range(steps):
            grad_copy(j).wait_send()

    ag_drain()
    for h in range(2):
        pair_copy(h).wait_send()
    rs_drain()
    gx.wait_send()
    ws_drain()
    wg_drain()


def shards(
    sections, n_dev,
    late_sent, entry_rows, gain_first, shift_first, expand_late, gain_inner, shift_inner,
    reduce_late, early_saved, upstream_grad, exit_grad, expand_early, reduce_early,
):
    rows, cl = entry_rows.shape
    e_rows, ce = exit_grad.shape
    fe = expand_early.shape[2]
    hid = expand_late.shape[2]
    Q = n_dev // 2
    half = cl // 2
    padded = -(-rows // 16) * 16
    chunk = max(k for k in range(16, 257, 16) if e_rows % k == 0)
    steps = e_rows // chunk
    depth = ce // Q
    any_spec = pl.BlockSpec(memory_space=pl.ANY)
    vm = pl.BlockSpec(memory_space=pltpu.VMEM)
    V = pltpu.VMEM
    dma = pltpu.SemaphoreType.DMA
    ring = [dma((2, Q - 1)), dma((2, Q - 1))]
    late_out, input_grad, gexp, gred = pl.pallas_call(
        functools.partial(kernel, sections, n_dev, chunk),
        out_shape=(
            jax.ShapeDtypeStruct((rows, cl), BF16),
            jax.ShapeDtypeStruct((e_rows, ce), BF16),
            jax.ShapeDtypeStruct((ce, fe), BF16),
            jax.ShapeDtypeStruct((fe, ce), BF16),
        ),
        in_specs=[any_spec, any_spec, vm, vm, any_spec, vm, vm] + [any_spec] * 6,
        out_specs=(vm, vm, vm, vm),
        scratch_shapes=[
            V((2, n_dev, rows, half), BF16),
            V((n_dev * padded, cl), BF16),
            V((n_dev * padded, hid), BF16),
            V((2, 2, Q, rows, half), BF16),
            V((2, Q, rows, half), BF16),
            V((2, Q - 1, rows, half), BF16),
            V((2, Q - 1, rows, half), BF16),
            V((cl, hid), BF16),
            V((hid, cl), BF16),
            V((e_rows, ce), BF16),
            V((e_rows, ce), BF16),
            V((ce, fe), BF16),
            V((fe, ce), BF16),
            V((e_rows, fe), BF16),
            V((e_rows, fe), F32),
            V((e_rows, fe), BF16),
            V((2, Q, depth, fe), F32),
            V((Q, depth, fe), BF16),
            V((Q, depth, fe), BF16),
            V((2, Q - 1, depth, fe // 2), BF16),
            V((2, Q - 1, depth, fe // 2), BF16),
            V((2, n_dev, depth, fe // 2), BF16),
            V((ce, fe), F32),
            dma((5,)), dma((2,)), dma((2,)), dma((steps,)), dma((steps,)),
            *ring, dma((2, Q)), dma((2, Q)), dma((2,)), dma((2,)), *ring,
            dma, dma, *ring, *ring, dma((2, Q)), dma((2, Q)),
        ],
        compiler_params=pltpu.CompilerParams(
            collective_id=0, has_side_effects=True, vmem_limit_bytes=60 * 1024 * 1024
        ),
        name="relay",
    )(
        late_sent[0], entry_rows, gain_first, shift_first, expand_late[0], gain_inner, shift_inner,
        reduce_late[0], early_saved[0], upstream_grad[0], exit_grad, expand_early[0], reduce_early[0],
    )
    return late_out[None], input_grad[None], gexp.astype(F32)[None], gred.astype(F32)[None]


def solution(mesh):
    sections, n_dev = mesh.shape["section"], mesh.shape["dev"]
    sd, dd = P("section", "dev", None), P("dev", None)
    rep, one = P("section", None, None), P("section", None)
    in_specs = (
        sd, dd, one, one, P("section", None, "dev"), P("section", "dev"), P("section", "dev"),
        sd, sd, sd, dd, rep, rep,
    )
    return jax.shard_map(
        functools.partial(shards, sections, n_dev), mesh=mesh, in_specs=in_specs,
        out_specs=(sd, sd, rep, rep), check_vma=False,
    )
```
